32 devices in a mesh: rows: 8 (over z, y), par: 4 (over x, core).
Axes of the slice: x: 2, y: 2, z: 4, core: 2. Of those that a mesh axis runs over, the one named last changes fastest.
Arguments:
- base_a: bfloat16 [4, 64, 256], P(None, 'rows'), may hold values from -6 to 6
- base_b: bfloat16 [4, 64, 256], P(None, 'rows'), may hold values from -6 to 6
- input_scale: float32 [256], replicated, may hold values from 0.1 to 3
- layer_one: bfloat16 [256, 1024], replicated, may hold values from -0.375 to 0.375
- layer_two: bfloat16 [1024, 1024], replicated, may hold values from -0.1875 to 0.1875
- layer_three: bfloat16 [1024, 128], replicated, may hold values from -0.1875 to 0.1875
- swap_cols: int32 [256], P('par'), may hold values from 0 to 255, each once
- window_ends: int32 [4], replicated, may hold values from 32 to 64
Outputs:
- first_order: float32 [4, 256, 128], P(None, 'par')
- total_order: float32 [4, 256, 128], P(None, 'par')
- total_variance: float32 [4, 128], replicated
The draws below stay inside these ranges and needn't reach their ends.
Inputs may be any that keep to these rules, and one draw needn't show every extreme that they name: window w uses its rows 0 to window_ends[w] - 1. `swap_cols`: each column appears once.
All inputs are finite; a program needn't handle non-finite values.
Results may differ from the reference program's by a relative error of at most 0.0055.
The reference program's roundings to bfloat16 on the way (of `inputs_a`, `inputs_b`, `inputs_c`, `hidden_one` and `hidden_two`) count: a program that leaves them out, or rounds other values in their place, can miss the bound.
Values sent between devices are 32-bit elements; how exact they have to be, the bound alone decides.
A program may use at most 64 MiB of HBM per device.

```python
import math
import jax
import jax.numpy as jnp
from jax import lax

D = 256
HIDDEN_SIZE = 1024
OUTPUTS = 128
WINDOWS = 4
WINDOW_ROWS = 64


def place_ends(values, key, least, top_value):
    longest = values.shape.index(max(values.shape))
    spots = []
    for shift in (0, 1):
        where = [jax.random.randint(jax.random.fold_in(key, axis), (), 0, length) for axis, length in enumerate(values.shape)]
        where[longest] = (where[longest] + shift) % values.shape[longest]
        spots.append(tuple(where))
    return values.at[spots[0]].set(least).at[spots[1]].set(top_value)


def block_scale(stream_key, extent, split, low, largest):
    def one(axis_at, shards_of):
        steps = jax.random.uniform(jax.random.fold_in(jax.random.fold_in(stream_key, 6), axis_at), (shards_of,), jnp.float32, low / len(split), largest / len(split))
        return jnp.repeat(jnp.exp(steps), extent[axis_at] // shards_of).reshape((-1,) + (1,) * (len(extent) - axis_at - 1))

    level = one(*split[0])
    for cut in split[1:]:
        level = level * one(*cut)
    return level


def noise(key, extent, spread, reach, split=(), held_as=jnp.bfloat16):
    entries = jax.random.normal(key, extent, jnp.float32) * spread
    if len(split) > 0:
        entries = block_scale(key, extent, split, -0.22, 0.18) * entries
    return jnp.clip(entries, min=-reach, max=reach).astype(held_as)


def setup_inputs(seed: int = 0) -> dict:
    key_of = jax.random.split(jax.random.key(seed), 9)
    base_a = noise(key_of[0], (WINDOWS, WINDOW_ROWS, D), 1.0, 6.0, ((1, 8),))
    base_b = noise(key_of[1], (WINDOWS, WINDOW_ROWS, D), 1.0, 6.0, ((1, 8),))
    input_scale = jnp.clip(jnp.exp(jax.random.uniform(key_of[2], (D,), jnp.float32, math.log(0.1), math.log(3.0))), 0.1, 3.0)
    layer_one = noise(key_of[3], (D, HIDDEN_SIZE), D ** -0.5, 0.375)
    layer_two = noise(key_of[4], (HIDDEN_SIZE, HIDDEN_SIZE), HIDDEN_SIZE ** -0.5, 0.1875)
    layer_three = noise(key_of[5], (HIDDEN_SIZE, OUTPUTS), HIDDEN_SIZE ** -0.5, 0.1875)
    swap_cols = jax.random.permutation(key_of[6], D).astype(jnp.int32)
    window_ends = place_ends(jax.random.randint(key_of[7], (WINDOWS,), WINDOW_ROWS // 2, WINDOW_ROWS + 1), jax.random.fold_in(key_of[7], 1), WINDOW_ROWS // 2, WINDOW_ROWS).astype(jnp.int32)
    return {"base_a": base_a, "base_b": base_b, "input_scale": input_scale, "layer_one": layer_one, "layer_two": layer_two, "layer_three": layer_three, "swap_cols": swap_cols, "window_ends": window_ends}


def network_tail(first_pre, layer_two, layer_three):
    hidden_one = jax.nn.silu(first_pre).astype(jnp.bfloat16)
    second_pre = jnp.dot(hidden_one, layer_two, preferred_element_type=jnp.float32)
    hidden_two = jax.nn.silu(second_pre).astype(jnp.bfloat16)
    return jnp.dot(hidden_two, layer_three, preferred_element_type=jnp.float32)


def surrogate(inputs, layer_one, layer_two, layer_three):
    first_pre = jnp.dot(inputs, layer_one, preferred_element_type=jnp.float32)
    return network_tail(first_pre, layer_two, layer_three)


def merge_total(former, latter):
    counts = former[0] + latter[0]
    change = latter[1] - former[1]
    return (counts, former[1] + change * latter[0] / counts,
            former[2] + latter[2] + change * change * former[0] * latter[0] / counts)


def merge_groups(former, latter):
    counts = former[0] + latter[0]
    change_b = latter[1] - former[1]
    change_d = latter[2] - former[2]
    pair_weight = former[0] * latter[0] / counts
    return (counts, former[1] + change_b * latter[0] / counts, former[2] + change_d * latter[0] / counts,
            former[3] + latter[3] + change_d * change_d * pair_weight,
            former[4] + latter[4] + change_b * change_d * pair_weight)


def reference(base_a, base_b, input_scale, layer_one, layer_two, layer_three, swap_cols, window_ends):
    positions = jnp.arange(D, dtype=jnp.int32)
    row_ids = jnp.arange(WINDOW_ROWS, dtype=jnp.int32)
    firsts = []
    totals = []
    variances = []
    running_total = None
    running_groups = None
    for window in range(WINDOWS):
        inputs_a = (base_a[window].astype(jnp.float32) * input_scale).astype(jnp.bfloat16)
        inputs_b = (base_b[window].astype(jnp.float32) * input_scale).astype(jnp.bfloat16)
        usable = (row_ids < window_ends[window]).astype(jnp.float32)[:, None]
        counts = jnp.sum(usable)
        out_a = surrogate(inputs_a, layer_one, layer_two, layer_three)
        out_b = surrogate(inputs_b, layer_one, layer_two, layer_three)
        pooled_count = 2.0 * counts
        pooled_mean = jnp.sum(usable * (out_a + out_b), axis=0) / pooled_count
        dev_a = out_a - pooled_mean
        dev_b = out_b - pooled_mean
        pooled_spread = jnp.sum(usable * (dev_a * dev_a + dev_b * dev_b), axis=0)
        mean_b = jnp.sum(usable * out_b, axis=0) / counts
        centered_b = usable * (out_b - mean_b)

        def one_group(column):
            chosen = (positions == column)[None, :]
            inputs_c = jnp.where(chosen, inputs_b, inputs_a)
            differ = surrogate(inputs_c, layer_one, layer_two, layer_three) - out_a
            mean_d = jnp.sum(usable * differ, axis=0) / counts
            centered_d = usable * (differ - mean_d)
            return mean_d, jnp.sum(centered_d * centered_d, axis=0), jnp.sum(centered_b * centered_d, axis=0)

        mean_d, spread_d, cross = lax.map(one_group, swap_cols)
        total_state = (pooled_count, pooled_mean, pooled_spread)
        group_state = (counts, mean_b, mean_d, spread_d, cross)
        if window == 0:
            running_total = total_state
            running_groups = group_state
        else:
            running_total = merge_total(running_total, total_state)
            running_groups = merge_groups(running_groups, group_state)
        variance = running_total[2] / running_total[0]
        firsts.append(running_groups[4] / running_groups[0] / variance)
        totals.append(0.5 * (running_groups[3] / running_groups[0] + running_groups[2] * running_groups[2]) / variance)
        variances.append(variance)
    return jnp.stack(firsts), jnp.stack(totals), jnp.stack(variances)
```

```python
import functools

import jax
import jax.numpy as jnp
from jax import lax
from jax.experimental import pallas as pl
from jax.experimental.pallas import tpu as pltpu
from jax.sharding import PartitionSpec as P

F32 = jnp.float32
BF16 = jnp.bfloat16
MESH = pl.DeviceIdType.MESH


def silu(value):
    half = 0.5 * value
    return half + half * jnp.tanh(half)


def dot(x, y):
    return jnp.dot(x, y, preferred_element_type=F32)


def dot_t(x, y):
    return lax.dot_general(x, y, (((1,), (1,)), ((), ())), preferred_element_type=F32)


def chunk_plan(n):
    unit = max(1, n // 8)
    sizes = [unit, unit, 2 * unit, 2 * unit, 2 * unit] if n >= 8 else [1] * n
    plan, start = [], 0
    for size in sizes:
        plan.append((start, size))
        start += size
    while start < n:
        plan.append((start, 1))
        start += 1
    return plan


def kernel(n, base_a, base_b, scale, cols, ends, w1_hbm, w2_hbm, w3_hbm,
           first, total, variance,
           w1, w2, w3, a_all, a_send, sel_all, sel_send, b_all, out_a_all, diff, onehot, h1, h2,
           w_sems, a_ss, a_rs, s_ss, s_rs, b_ss, b_rs, f_ss, f_rs, t_ss, t_rs):
    windows, window_rows, width = base_a.shape
    gq = first.shape[2]
    padded = onehot.shape[1]
    hidden = w2.shape[0]
    outputs = w3.shape[1]
    rows = windows * window_rows
    me = lax.axis_index("rows")

    loads = [pltpu.make_async_copy(src, dst, w_sems.at[i])
             for i, (src, dst) in enumerate(((w1_hbm, w1), (w2_hbm, w2), (w3_hbm, w3)))]
    for load in loads:
        load.start()

    barrier = pltpu.get_barrier_semaphore()
    for k in range(1, n):
        pl.semaphore_signal(barrier, inc=1, device_id={"rows": lax.rem(me + k, n)}, device_id_type=MESH)

    def send(src, dst, ss, rs, k):
        return pltpu.make_async_remote_copy(
            src_ref=src, dst_ref=dst, send_sem=ss.at[k], recv_sem=rs.at[k],
            device_id={"rows": lax.rem(me + n - k, n)}, device_id_type=MESH)

    factor = scale[...]
    own_a32 = (base_a[...].reshape(rows, width).astype(F32) * factor).astype(BF16).astype(F32)
    own_b = (base_b[...].reshape(rows, width).astype(F32) * factor).astype(BF16)
    a_send[...] = own_a32
    a_all[0] = own_a32
    lane = lax.broadcasted_iota(jnp.int32, (padded, width), 1)
    sub = lax.broadcasted_iota(jnp.int32, (padded, width), 0)
    for r in range(n):
        wanted = jnp.full((padded, width), cols[r * gq], jnp.int32)
        for g in range(1, gq):
            wanted = jnp.where(sub == g, cols[r * gq + g], wanted)
        onehot[r] = (lane == wanted).astype(F32)
    marks = onehot[...].reshape(n * padded, width).astype(BF16)
    chosen_b = dot_t(marks, own_b)
    sel_send[...] = chosen_b.reshape(n, padded, rows)
    sel_all[0] = sel_send[me]
    mark_own = onehot[me].astype(BF16)

    pl.semaphore_wait(barrier, n - 1)
    a_copies, s_copies = [], []
    for k in range(1, n):
        a_copies.append(send(a_send, a_all.at[k], a_ss, a_rs, k))
        a_copies[-1].start()
        s_copies.append(send(sel_send.at[lax.rem(me + n - k, n)], sel_all.at[k], s_ss, s_rs, k))
        s_copies[-1].start()

    loads[0].wait()
    swapped = dot(mark_own, w1[...])

    def tail(count):
        for c in range(0, hidden, 256):
            h2[:count, c : c + 256] = silu(dot(h1[:count, :], w2[:, c : c + 256])).astype(BF16)
        return dot(h2[:count, :], w3[...])

    b_copies = []
    for start, size in chunk_plan(n):
        if start > 0:
            for k in range(start, start + size):
                a_copies[k - 1].wait_recv()
                s_copies[k - 1].wait_recv()
        a_chunk = a_all[start : start + size].reshape(size * rows, width).astype(BF16)
        pre = dot(a_chunk, w1[...])
        chosen_a = dot_t(a_chunk, mark_own)
        base = 0
        for s in range(size):
            pre_s = pre[s * rows : (s + 1) * rows]
            delta = jnp.transpose(sel_all[start + s]) - chosen_a[s * rows : (s + 1) * rows]
            for g in range(gq):
                value = pre_s + delta[:, g : g + 1] * swapped[g : g + 1, :]
                h1[base : base + rows, :] = silu(value).astype(BF16)
                base += rows
            h1[base : base + rows, :] = silu(pre_s).astype(BF16)
            base += rows
        if start == 0:
            h1[base : base + rows, :] = silu(dot(own_b, w1[...])).astype(BF16)
            base += rows
            loads[1].wait()
            loads[2].wait()
        out = tail(base)
        base = 0
        for s in range(size):
            out_a = out[base + gq * rows : base + (gq + 1) * rows]
            out_a_all[start + s] = out_a
            for g in range(gq):
                diff[g, start + s] = out[base : base + rows] - out_a
                base += rows
            base += rows
        if start == 0:
            b_all[0] = out[base : base + rows]
            for k in range(1, n):
                b_copies.append(send(b_all.at[0], b_all.at[k], b_ss, b_rs, k))
                b_copies[-1].start()
    for copy in b_copies:
        copy.wait_recv()

    row_id = lax.broadcasted_iota(jnp.int32, (n, window_rows, outputs), 1)
    slot = lax.broadcasted_iota(jnp.int32, (n, window_rows, outputs), 0)
    position = lax.rem(me + slot, n) * window_rows + row_id
    former = None
    for w in range(windows):
        span = slice(w * window_rows, (w + 1) * window_rows)
        usable = (position < ends[w]).astype(F32)
        counts = jnp.full((1, outputs), ends[w], jnp.int32).astype(F32)
        inverse = 1.0 / counts
        oa = out_a_all[:, span, :]
        ob = b_all[:, span, :]

        def over_rows(x):
            return jnp.sum(jnp.sum(x, axis=0), axis=0, keepdims=True)

        pooled_mean = over_rows(usable * (oa + ob)) * (0.5 * inverse)
        dev_a = oa - pooled_mean
        dev_b = ob - pooled_mean
        pooled_spread = over_rows(usable * (dev_a * dev_a + dev_b * dev_b))
        mean_b = over_rows(usable * ob) * inverse
        centred_b = usable * (ob - mean_b)
        means, spreads, crosses = [], [], []
        for g in range(gq):
            d = diff[g, :, span, :]
            mean_d = over_rows(usable * d) * inverse
            centred = usable * (d - mean_d)
            means.append(mean_d)
            spreads.append(over_rows(centred * centred))
            crosses.append(over_rows(centred_b * centred))
        now = (counts, pooled_mean, pooled_spread, mean_b, jnp.concatenate(means, 0),
               jnp.concatenate(spreads, 0), jnp.concatenate(crosses, 0))
        if former is not None:
            n1, n2 = former[0], counts
            both = n1 + n2
            share = n2 / both
            weight = n1 * share
            e_p = now[1] - former[1]
            e_b = now[3] - former[3]
            e_d = now[4] - former[4]
            now = (both, former[1] + e_p * share, former[2] + now[2] + 2.0 * weight * e_p * e_p,
                   former[3] + e_b * share, former[4] + e_d * share,
                   former[5] + now[5] + e_d * e_d * weight, former[6] + now[6] + e_b * e_d * weight)
        former = now
        spread = now[2] / (2.0 * now[0])
        first[w, me] = now[6] / now[0] / spread
        total[w, me] = 0.5 * (now[5] / now[0] + now[4] * now[4]) / spread
        variance[w : w + 1, :] = spread

    f_copies = []
    for k in range(1, n):
        for ref, ss, rs in ((first, f_ss, f_rs), (total, t_ss, t_rs)):
            f_copies.append(send(ref.at[:, me], ref.at[:, me], ss, rs, k))
            f_copies[-1].start()
    for copy in f_copies:
        copy.wait_recv()
    for copy in a_copies + s_copies + b_copies + f_copies:
        copy.wait_send()


def solution(mesh):
    n = mesh.shape["rows"]

    def local(base_a, base_b, input_scale, layer_one, layer_two, layer_three, swap_cols, window_ends):
        windows, window_rows, width = base_a.shape
        groups = swap_cols.shape[0]
        gq = groups // n
        padded = -(-gq // 8) * 8
        hidden = layer_two.shape[0]
        outputs = layer_three.shape[1]
        rows = windows * window_rows
        most = max((size * (gq + 1) + (start == 0)) * rows for start, size in chunk_plan(n))
        vmem = pl.BlockSpec(memory_space=pltpu.VMEM)
        smem = pl.BlockSpec(memory_space=pltpu.SMEM)
        hbm = pl.BlockSpec(memory_space=pl.ANY)
        dma = pltpu.SemaphoreType.DMA
        first, total, variance = pl.pallas_call(
            functools.partial(kernel, n),
            out_shape=(
                jax.ShapeDtypeStruct((windows, n, gq, outputs), F32),
                jax.ShapeDtypeStruct((windows, n, gq, outputs), F32),
                jax.ShapeDtypeStruct((windows, outputs), F32),
            ),
            in_specs=[vmem, vmem, vmem, smem, smem, hbm, hbm, hbm],
            out_specs=(vmem, vmem, vmem),
            scratch_shapes=[
                pltpu.VMEM(layer_one.shape, BF16),
                pltpu.VMEM(layer_two.shape, BF16),
                pltpu.VMEM(layer_three.shape, BF16),
                pltpu.VMEM((n, rows, width), F32),
                pltpu.VMEM((rows, width), F32),
                pltpu.VMEM((n, padded, rows), F32),
                pltpu.VMEM((n, padded, rows), F32),
                pltpu.VMEM((n, rows, outputs), F32),
                pltpu.VMEM((n, rows, outputs), F32),
                pltpu.VMEM((gq, n, rows, outputs), F32),
                pltpu.VMEM((n, padded, width), F32),
                pltpu.VMEM((most, hidden), BF16),
                pltpu.VMEM((most, hidden), BF16),
                dma((3,)),
            ] + [dma((n,)) for _ in range(10)],
            compiler_params=pltpu.CompilerParams(
                collective_id=0, has_side_effects=True, vmem_limit_bytes=56 * 2**20
            ),
        )(base_a, base_b, input_scale.reshape(1, width), swap_cols, window_ends,
          layer_one, layer_two, layer_three)
        shape = (windows, groups, outputs)
        return first.reshape(shape), total.reshape(shape), variance

    in_specs = (P(None, "rows", None), P(None, "rows", None), P(), P(), P(), P(), P("par"), P())
    out_specs = (P(None, "par", None), P(None, "par", None), P())
    return jax.shard_map(local, mesh=mesh, in_specs=in_specs, out_specs=out_specs, check_vma=False)
```
